32 devices in a mesh: gz: 8 (over z, y), gy: 4 (over x, core).
Axes of the slice: x: 2, y: 2, z: 4, core: 2. Of those that a mesh axis runs over, the one named last changes fastest.
Arguments:
- density: float32 [64, 123904], P('gz', 'gy'), may hold values from -6 to 6
Outputs:
- potential: float32 [64, 123904], P('gz', 'gy')
The draws below stay inside these ranges and needn't reach their ends.
All inputs are finite; a program needn't handle non-finite values.
Results may differ from the reference program's by a relative error of at most 0.00014.
Values sent between devices are 32-bit elements; how exact they have to be, the bound alone decides.
A program may use at most 128 MiB of HBM per device.

```python
import math
import jax
import jax.numpy as jnp
from jax import lax

NX = 352
NY = 352
SCREEN = 128
NZ = 64


def block_levels(stream_key, dims, pieces, least, high):
    factor_of, own = 1.0, jax.random.fold_in(stream_key, 6)
    for position, parts in pieces:
        heights = jnp.exp(jax.random.uniform(jax.random.fold_in(own, position), (parts,), jnp.float32, least / len(pieces), high / len(pieces)))
        factor_of = factor_of * jnp.repeat(heights, dims[position] // parts).reshape([-1 if axis == position else 1 for axis in range(len(dims))])
    return factor_of


def normal_values(own_key, shape, scale, bound, split=(), held_as=jnp.bfloat16):
    array = scale * jax.random.normal(own_key, shape, jnp.float32)
    if split:
        array = array * block_levels(own_key, shape, split, -0.22, 0.18)
    return jnp.clip(array, -bound, bound).astype(held_as)


def setup_inputs(seed: int = 0) -> dict:
    keys = jax.random.split(jax.random.key(seed), 2)
    return {
        "density": normal_values(keys[0], (NZ, NY * NX), 1.0, 6.0, ((0, 8), (1, 4)), jnp.float32),
    }


def reference(density):
    planes = density.shape[0]
    width_x = NX
    width_y = NY
    field = jnp.transpose(density.reshape(planes, width_y, width_x), (0, 2, 1))
    hat = jnp.fft.rfft2(field, axes=(1, 2))
    index_x = jnp.arange(width_x, dtype=jnp.int32)
    wave_x = jnp.minimum(index_x, width_x - index_x).astype(jnp.float32) * (2.0 * math.pi / width_x)
    wave_y = jnp.arange(width_y // 2 + 1, dtype=jnp.int32).astype(jnp.float32) * (2.0 * math.pi / width_y)
    kappa = jnp.sqrt(1.0 / (SCREEN * SCREEN) + wave_x[:, None] ** 2 + wave_y[None, :] ** 2)
    decay = jnp.exp(-kappa)

    def forward(carry, plane):
        carry = decay * carry + plane
        return (carry, carry)

    def backward(carry, plane):
        return (decay * (carry + plane), carry)
    _, upward = lax.scan(forward, jnp.zeros_like(hat[0]), hat)
    _, downward = lax.scan(backward, jnp.zeros_like(hat[0]), hat, reverse=True)
    phi = (upward + downward) * (0.5 / kappa)
    result = jnp.fft.irfft2(phi, s=(width_x, width_y), axes=(1, 2)).astype(jnp.float32)
    return jnp.transpose(result, (0, 2, 1)).reshape(planes, width_y * width_x)
```

```python
import functools
import math

import jax
import jax.numpy as jnp
import numpy as np
from jax import lax
from jax.experimental import pallas as pl
from jax.experimental.pallas import tpu as pltpu
from jax.sharding import PartitionSpec as P

NX = 352
NY = 352
SCREEN = 128
LANES = 128
MESH = pl.DeviceIdType.MESH


def basis(length):
    j = np.arange(length)
    half = length // 2
    m = np.where(j <= half, j, j - half)
    angle = (m[:, None] * j[None, :] % length) * (2.0 * math.pi / length)
    rows = np.where(j[:, None] <= half, np.cos(angle), np.sin(angle))
    amp = np.where((j == 0) | (j == half), math.sqrt(1.0 / length), math.sqrt(2.0 / length))
    return rows * amp[:, None]


def split(value):
    high = value.astype(jnp.bfloat16)
    low = (value - high.astype(jnp.float32)).astype(jnp.bfloat16)
    return high, low


def dot3(a, b):
    dot = functools.partial(jnp.dot, preferred_element_type=jnp.float32)
    return dot(a[0], b[0]) + (dot(a[0], b[1]) + dot(a[1], b[0]))


def kappa_of(rows, first_row, lanes, first_lane):
    def wave(shape, axis, first, length):
        index = lax.broadcasted_iota(jnp.int32, shape, axis) + first
        index = jnp.where(index <= length // 2, index, index - length // 2)
        return index.astype(jnp.float32) * (2.0 * math.pi / length)

    wave_y = wave((rows, lanes), 0, first_row, NY)
    wave_x = wave((rows, lanes), 1, first_lane, NX)
    return jnp.sqrt(1.0 / (SCREEN * SCREEN) + wave_x * wave_x + wave_y * wave_y)


def kernel(planes, rows_y, gz, gy, part, density, fx, fx_low, ix, ix_low, fy, fy_low, iy, iy_low,
           out, rows_ref, slab, send, recv, hat, seg, total, edge, edge_all, carry, carry_all,
           back, send_sem, recv_sem, own_sem, edge_send, edge_recv, carry_send, carry_recv,
           back_send, back_recv):
    width = NX // gy
    pad = LANES
    me_z = lax.axis_index("gz")
    me_y = lax.axis_index("gy")
    barrier = pltpu.get_barrier_semaphore()
    for i in range(1, gy):
        pl.semaphore_signal(barrier, inc=1, device_id=(me_z, lax.rem(me_y + i, gy)), device_id_type=MESH)
    for i in range(1, gz):
        pl.semaphore_signal(barrier, inc=1, device_id=(lax.rem(me_z + i, gz), me_y), device_id_type=MESH)

    period = LANES // math.gcd(NX, LANES)
    stretch = period * NX
    steps = rows_y // period
    tall = rows_y * planes
    chunks = [min(LANES, NX - c) for c in range(0, NX, LANES)]

    def unpack(t, _):
        base = pl.multiple_of(t * stretch, LANES)
        values = density[:, pl.ds(base, stretch)]
        for q in range(period):
            row = pl.multiple_of((t * period + q) * planes, planes)
            for c, size in enumerate(chunks):
                start = q * NX + c * LANES
                rows_ref[pl.ds(c * tall + row, planes), :size] = values[:, start:start + size]
        return 0

    lax.fori_loop(0, steps, unpack, 0)
    for z in range(planes):
        for c, size in enumerate(chunks):
            slab[z * rows_y:(z + 1) * rows_y, c * LANES:c * LANES + size] = rows_ref[
                pl.ds(c * tall + z, rows_y, stride=planes), :][:, :size]
    group = 2
    for z0 in range(0, planes, group):
        block = slab[z0 * rows_y:(z0 + group) * rows_y, :NX]
        result = dot3(split(block), (fx[...], fx_low[...]))
        for z in range(z0, z0 + group):
            for p in range(gy):
                send[p, :, z * width:(z + 1) * width] = result[
                    (z - z0) * rows_y:(z - z0 + 1) * rows_y, p * pad:p * pad + width]

    pl.semaphore_wait(barrier, gy - 1 + gz - 1)

    def exchange(source, target, sems, recvs):
        copies = []
        for i in list(range(2, gy)) + [1]:
            peer = lax.rem(me_y + i, gy)
            copy = pltpu.make_async_remote_copy(
                src_ref=source.at[peer], dst_ref=target.at[me_y],
                send_sem=sems.at[i], recv_sem=recvs.at[i],
                device_id=(me_z, peer), device_id_type=MESH)
            copy.start()
            copies.append(copy)
        own = pltpu.make_async_copy(source.at[me_y], target.at[me_y], own_sem)
        own.start()
        own.wait()
        for copy in copies:
            copy.wait()

    exchange(send, recv, send_sem, recv_sem)

    lanes = planes * width
    hat[...] = dot3((fy[...], fy_low[...]), split(recv[...].reshape(gy * rows_y, lanes)))
    rows = gz * part
    kappa = kappa_of(rows, 0, width, me_y * width)
    decay = jnp.exp(-kappa)
    value = None
    for z in range(planes):
        plane = hat[:, z * width:(z + 1) * width]
        seg[z] = plane
        value = plane if z == 0 else decay * value + plane
    edge[0] = value
    for z in range(planes - 1, -1, -1):
        value = seg[z] if z == planes - 1 else decay * value + seg[z]
    edge[1] = value

    copies = []
    mine = pl.ds(pl.multiple_of(me_z * part, part), part)
    for i in range(1, gz):
        peer = lax.rem(me_z + i, gz)
        copy = pltpu.make_async_remote_copy(
            src_ref=edge.at[:, pl.ds(pl.multiple_of(peer * part, part), part)],
            dst_ref=edge_all.at[me_z],
            send_sem=edge_send.at[i], recv_sem=edge_recv.at[i],
            device_id=(peer, me_y), device_id_type=MESH)
        copy.start()
        copies.append(copy)
    edge_all[me_z] = edge[:, mine]
    far = jnp.exp(-float(planes) * kappa_of(part, me_z * part, width, me_y * width))
    for copy in copies:
        copy.wait()
    value = jnp.zeros((part, width), jnp.float32)
    for s in range(gz):
        carry[s, 0] = value
        value = far * value + edge_all[s, 0]
    value = jnp.zeros((part, width), jnp.float32)
    for s in range(gz - 1, -1, -1):
        carry[s, 1] = value
        value = far * value + edge_all[s, 1]
    copies = []
    for i in range(1, gz):
        peer = lax.rem(me_z + i, gz)
        copy = pltpu.make_async_remote_copy(
            src_ref=carry.at[peer], dst_ref=carry_all.at[:, mine],
            send_sem=carry_send.at[i], recv_sem=carry_recv.at[i],
            device_id=(peer, me_y), device_id_type=MESH)
        copy.start()
        copies.append(copy)
    carry_all[:, mine] = carry[me_z]
    for copy in copies:
        copy.wait()

    scale = 0.5 / kappa
    value = carry_all[0]
    for z in range(planes):
        value = decay * value + seg[z]
        total[z] = value
    value = carry_all[1]
    for z in range(planes - 1, -1, -1):
        value = decay * value
        hat[:, z * width:(z + 1) * width] = (total[z] + value) * scale
        value = value + seg[z]

    result = dot3((iy[...], iy_low[...]), split(hat[...]))
    for p in range(gy):
        send[p] = result[p * rows_y:(p + 1) * rows_y]
    exchange(send, back, back_send, back_recv)

    slab[...] = jnp.zeros_like(slab)
    for z in range(planes):
        for p in range(gy):
            slab[z * rows_y:(z + 1) * rows_y, p * pad:p * pad + width] = back[
                p, :, z * width:(z + 1) * width]
    for z0 in range(0, planes, group):
        block = slab[z0 * rows_y:(z0 + group) * rows_y, :]
        result = dot3(split(block), (ix[...], ix_low[...]))
        for z in range(z0, z0 + group):
            for c in range(len(chunks)):
                rows_ref[pl.ds(c * tall + z, rows_y, stride=planes), :] = result[
                    (z - z0) * rows_y:(z - z0 + 1) * rows_y, c * LANES:(c + 1) * LANES]

    def pack(t, _):
        pieces = []
        for q in range(period):
            row = pl.multiple_of((t * period + q) * planes, planes)
            for c, size in enumerate(chunks):
                pieces.append(rows_ref[pl.ds(c * tall + row, planes), :][:, :size])
        base = pl.multiple_of(t * stretch, LANES)
        out[:, pl.ds(base, stretch)] = jnp.concatenate(pieces, axis=1)
        return 0

    lax.fori_loop(0, steps, pack, 0)


def on_device(density):
    planes = density.shape[0]
    gz = lax.axis_size("gz")
    gy = lax.axis_size("gy")
    rows_y = NY // gy
    width = NX // gy
    part = -(-NY // (8 * gz)) * 8
    rows = part * gz
    forward_x = np.zeros((NX, gy, LANES))
    forward_x[:, :, :width] = basis(NX).T.reshape(NX, gy, width)
    forward_x = forward_x.reshape(NX, gy * LANES)
    forward_y = np.zeros((rows, NY))
    forward_y[:NY] = basis(NY)
    tables = []
    inverse_x = np.zeros((gy * LANES, -(-NX // LANES) * LANES))
    inverse_x[:, :NX] = forward_x.T
    for table in (forward_x, inverse_x, forward_y, forward_y.T):
        table = table.astype(np.float32)
        high = table.astype(jnp.bfloat16)
        low = (table - high.astype(np.float32)).astype(jnp.bfloat16)
        tables += [high, low]
    f32 = jnp.float32
    vmem = pltpu.VMEM
    dma = pltpu.SemaphoreType.DMA
    lanes = planes * width
    spec = pl.BlockSpec(memory_space=pltpu.VMEM)
    return pl.pallas_call(
        functools.partial(kernel, planes, rows_y, gz, gy, part),
        out_shape=jax.ShapeDtypeStruct(density.shape, f32),
        in_specs=[spec] * (1 + len(tables)),
        out_specs=spec,
        scratch_shapes=[
            vmem((-(-NX // LANES) * rows_y * planes, LANES), f32),
            vmem((rows_y * planes, gy * LANES), f32),
            vmem((gy, rows_y, lanes), f32),
            vmem((gy, rows_y, lanes), f32),
            vmem((rows, lanes), f32),
            vmem((planes, rows, width), f32),
            vmem((planes, rows, width), f32),
            vmem((2, rows, width), f32),
            vmem((gz, 2, part, width), f32),
            vmem((gz, 2, part, width), f32),
            vmem((2, rows, width), f32),
            vmem((gy, rows_y, lanes), f32),
            dma((gy,)), dma((gy,)), dma(()),
            dma((gz,)), dma((gz,)), dma((gz,)), dma((gz,)),
            dma((gy,)), dma((gy,)),
        ],
        compiler_params=pltpu.CompilerParams(
            collective_id=0, has_side_effects=True, vmem_limit_bytes=60 * 1024 * 1024),
    )(density, *tables)


def solution(mesh):
    return jax.shard_map(
        on_device,
        mesh=mesh,
        in_specs=(P("gz", "gy"),),
        out_specs=P("gz", "gy"),
        check_vma=False,
    )
```

```python
import functools
import math

import jax
import jax.numpy as jnp
import numpy as np
from jax import lax
from jax.experimental import pallas as pl
from jax.experimental.pallas import tpu as pltpu
from jax.sharding import PartitionSpec as P

NX = 352
NY = 352
SCREEN = 128
LANES = 128
MESH = pl.DeviceIdType.MESH


def basis(length):
    j = np.arange(length)
    half = length // 2
    m = np.where(j <= half, j, j - half)
    angle = (m[:, None] * j[None, :] % length) * (2.0 * math.pi / length)
    rows = np.where(j[:, None] <= half, np.cos(angle), np.sin(angle))
    amp = np.where((j == 0) | (j == half), math.sqrt(1.0 / length), math.sqrt(2.0 / length))
    return rows * amp[:, None]


def split(value):
    high = value.astype(jnp.bfloat16)
    low = (value - high.astype(jnp.float32)).astype(jnp.bfloat16)
    return high, low


def dot3(a, b):
    dot = functools.partial(jnp.dot, preferred_element_type=jnp.float32)
    return dot(a[0], b[0]) + (dot(a[0], b[1]) + dot(a[1], b[0]))


def kappa_of(rows, first_row, lanes, first_lane):
    def wave(shape, axis, first, length):
        index = lax.broadcasted_iota(jnp.int32, shape, axis) + first
        index = jnp.where(index <= length // 2, index, index - length // 2)
        return index.astype(jnp.float32) * (2.0 * math.pi / length)

    wave_y = wave((rows, lanes), 0, first_row, NY)
    wave_x = wave((rows, lanes), 1, first_lane, NX)
    return jnp.sqrt(1.0 / (SCREEN * SCREEN) + wave_x * wave_x + wave_y * wave_y)


def kernel(planes, rows_y, gz, gy, part, parts, density, *refs):
    tables_hbm, refs = refs[:8], refs[8:]
    (out, rows_ref, slab, cols, acc, out_buf, send, recv, hat, seg, total, edge, edge_all, carry,
     carry_all, send_back, back, decay_ref, scale_ref, *refs) = refs
    tables, refs = refs[:8], refs[8:]
    (table_sem, own_sem, out_sem, send_sem, recv_sem, edge_send, edge_recv, carry_send, carry_recv,
     back_send, back_recv) = refs
    fx, fx_low, ix, ix_low, fy, fy_low, iy, iy_low = tables
    half = NX // gy // parts
    slot = LANES // parts
    me_z = lax.axis_index("gz")
    me_y = lax.axis_index("gy")
    loads = []
    for i in range(8):
        load = pltpu.make_async_copy(tables_hbm[i], tables[i], table_sem.at[i])
        load.start()
        loads.append(load)
    barrier = pltpu.get_barrier_semaphore()
    for i in range(1, gy):
        pl.semaphore_signal(barrier, inc=1, device_id=(me_z, lax.rem(me_y + i, gy)), device_id_type=MESH)
    for i in range(1, gz):
        pl.semaphore_signal(barrier, inc=1, device_id=(lax.rem(me_z + i, gz), me_y), device_id_type=MESH)

    period = LANES // math.gcd(NX, LANES)
    stretch = period * NX
    steps = rows_y // period
    tall = rows_y * planes
    chunks = [min(LANES, NX - c) for c in range(0, NX, LANES)]

    def unpack(t, _):
        base = pl.multiple_of(t * stretch, LANES)
        values = density[:, pl.ds(base, stretch)]
        for q in range(period):
            row = pl.multiple_of((t * period + q) * planes, planes)
            for c, size in enumerate(chunks):
                start = q * NX + c * LANES
                rows_ref[pl.ds(c * tall + row, planes), :size] = values[:, start:start + size]
        return 0

    lax.fori_loop(0, steps, unpack, 0)
    for z in range(planes):
        for c, size in enumerate(chunks):
            slab[z * rows_y:(z + 1) * rows_y, c * LANES:c * LANES + size] = rows_ref[
                pl.ds(c * tall + z, rows_y, stride=planes), :][:, :size]
    group = 2
    mine = pl.ds(pl.multiple_of(me_z * part, part), part)

    def forward_x(h):
        for z0 in range(0, planes, group):
            block = slab[z0 * rows_y:(z0 + group) * rows_y, :NX]
            result = dot3(split(block), (fx[h], fx_low[h]))
            for z in range(z0, z0 + group):
                for p in range(gy):
                    send[h, p, :, z * half:(z + 1) * half] = result[
                        (z - z0) * rows_y:(z - z0 + 1) * rows_y, p * slot:p * slot + half]

    def exchange(source, target, h, sems, recvs):
        copies = []
        for i in list(range(2, gy)) + [1]:
            peer = lax.rem(me_y + i, gy)
            copy = pltpu.make_async_remote_copy(
                src_ref=source.at[h, peer], dst_ref=target.at[h, me_y],
                send_sem=sems.at[h, i], recv_sem=recvs.at[h, i],
                device_id=(me_z, peer), device_id_type=MESH)
            copy.start()
            copies.append(copy)
        own = pltpu.make_async_copy(source.at[h, me_y], target.at[h, me_y], own_sem)
        own.start()
        own.wait()
        return copies

    def arrive(copies):
        for copy in copies:
            copy.wait()

    def edges(h):
        lanes = planes * half
        hat[...] = dot3((fy[...], fy_low[...]), split(recv[h].reshape(gy * rows_y, lanes)))
        decay = decay_ref[h]
        value = None
        for z in range(planes):
            plane = hat[:, z * half:(z + 1) * half]
            seg[h, z] = plane
            value = plane if z == 0 else decay * value + plane
        edge[h, :, :half] = value
        for z in range(planes - 1, -1, -1):
            value = seg[h, z] if z == planes - 1 else decay * value + seg[h, z]
        edge[h, :, half:2 * half] = value
        copies = []
        for i in range(1, gz):
            peer = lax.rem(me_z + i, gz)
            copy = pltpu.make_async_remote_copy(
                src_ref=edge.at[h, pl.ds(pl.multiple_of(peer * part, part), part)],
                dst_ref=edge_all.at[h, me_z],
                send_sem=edge_send.at[h, i], recv_sem=edge_recv.at[h, i],
                device_id=(peer, me_y), device_id_type=MESH)
            copy.start()
            copies.append(copy)
        edge_all[h, me_z] = edge[h, mine]
        return copies

    def carries(h):
        far = kappa_of(part, me_z * part, half, (me_y * parts + h) * half)
        far = jnp.exp(-float(planes) * far)
        value = jnp.zeros((part, half), jnp.float32)
        for s in range(gz):
            carry[h, s, :, :half] = value
            value = far * value + edge_all[h, s, :, :half]
        value = jnp.zeros((part, half), jnp.float32)
        for s in range(gz - 1, -1, -1):
            carry[h, s, :, half:2 * half] = value
            value = far * value + edge_all[h, s, :, half:2 * half]
        copies = []
        for i in range(1, gz):
            peer = lax.rem(me_z + i, gz)
            copy = pltpu.make_async_remote_copy(
                src_ref=carry.at[h, peer], dst_ref=carry_all.at[h, mine],
                send_sem=carry_send.at[h, i], recv_sem=carry_recv.at[h, i],
                device_id=(peer, me_y), device_id_type=MESH)
            copy.start()
            copies.append(copy)
        carry_all[h, mine] = carry[h, me_z]
        return copies

    def inverse_y(h):
        decay = decay_ref[h]
        scale = scale_ref[h]
        value = carry_all[h, :, :half]
        for z in range(planes):
            value = decay * value + seg[h, z]
            total[z] = value
        value = carry_all[h, :, half:2 * half]
        for z in range(planes - 1, -1, -1):
            value = decay * value
            hat[:, z * half:(z + 1) * half] = (total[z] + value) * scale
            value = value + seg[h, z]
        result = dot3((iy[...], iy_low[...]), split(hat[...]))
        for p in range(gy):
            send_back[h, p] = result[p * rows_y:(p + 1) * rows_y]

    def inverse_x(h):
        for z0 in range(0, planes, group):
            for z in range(z0, z0 + group):
                for p in range(gy):
                    cols[z * rows_y:(z + 1) * rows_y, p * slot:p * slot + half] = back[
                        h, p, :, z * half:(z + 1) * half]
            block = pl.ds(z0 * rows_y, group * rows_y)
            result = dot3(split(cols[block, :]), (ix[h], ix_low[h]))
            if h > 0:
                result = result + acc[block, :]
            if h < parts - 1:
                acc[block, :] = result
                continue
            for z in range(z0, z0 + group):
                for c in range(len(chunks)):
                    rows_ref[pl.ds(c * tall + z, rows_y, stride=planes), :] = result[
                        (z - z0) * rows_y:(z - z0 + 1) * rows_y, c * LANES:(c + 1) * LANES]

    loads[0].wait()
    loads[1].wait()
    moving = []
    for h in range(parts):
        forward_x(h)
        if h == 0:
            pl.semaphore_wait(barrier, gy - 1 + gz - 1)
        moving.append(exchange(send, recv, h, send_sem, recv_sem))
    for h in range(parts):
        kappa = kappa_of(gz * part, 0, half, (me_y * parts + h) * half)
        decay_ref[h] = jnp.exp(-kappa)
        scale_ref[h] = 0.5 / kappa
    edge[...] = jnp.zeros_like(edge)
    carry[...] = jnp.zeros_like(carry)
    cols[...] = jnp.zeros_like(cols)
    for i in range(2, 8):
        loads[i].wait()
    sent = []
    for h in range(parts):
        arrive(moving[h])
        sent.append(edges(h))
    returned = []
    for h in range(parts):
        arrive(sent[h])
        returned.append(carries(h))
    moving = []
    for h in range(parts):
        arrive(returned[h])
        inverse_y(h)
        moving.append(exchange(send_back, back, h, back_send, back_recv))
    for h in range(parts):
        arrive(moving[h])
        inverse_x(h)

    def pack(t, _):
        pieces = []
        for q in range(period):
            row = pl.multiple_of((t * period + q) * planes, planes)
            for c, size in enumerate(chunks):
                pieces.append(rows_ref[pl.ds(c * tall + row, planes), :][:, :size])
        base = pl.multiple_of(t * stretch, LANES)
        out_buf[:, pl.ds(base, stretch)] = jnp.concatenate(pieces, axis=1)
        return 0

    stores = []
    cuts = [0, steps // 2, steps]
    for i in range(2):
        lax.fori_loop(cuts[i], cuts[i + 1], pack, 0)
        span = pl.ds(cuts[i] * stretch, (cuts[i + 1] - cuts[i]) * stretch)
        store = pltpu.make_async_copy(out_buf.at[:, span], out.at[:, span], out_sem.at[i])
        store.start()
        stores.append(store)
    for store in stores:
        store.wait()


def on_device(density):
    planes = density.shape[0]
    gz = lax.axis_size("gz")
    gy = lax.axis_size("gy")
    parts = 2
    rows_y = NY // gy
    half = NX // gy // parts
    slot = LANES // parts
    part = -(-NY // (8 * gz)) * 8
    rows = part * gz
    wide = -(-NX // LANES) * LANES
    forward_x = np.zeros((parts, NX, gy, slot))
    forward_x[..., :half] = basis(NX).T.reshape(NX, gy, parts, half).transpose(2, 0, 1, 3)
    forward_x = forward_x.reshape(parts, NX, gy * slot)
    inverse_x = np.zeros((parts, gy * slot, wide))
    inverse_x[..., :NX] = forward_x.transpose(0, 2, 1)
    forward_y = np.zeros((rows, NY))
    forward_y[:NY] = basis(NY)
    tables = []
    for table in (forward_x, inverse_x, forward_y, forward_y.T):
        table = table.astype(np.float32)
        high = table.astype(jnp.bfloat16)
        low = (table - high.astype(np.float32)).astype(jnp.bfloat16)
        tables += [high, low]
    f32 = jnp.float32
    vmem = pltpu.VMEM
    dma = pltpu.SemaphoreType.DMA
    lanes = planes * half
    spec = pl.BlockSpec(memory_space=pltpu.VMEM)
    free = pl.BlockSpec(memory_space=pl.ANY)
    return pl.pallas_call(
        functools.partial(kernel, planes, rows_y, gz, gy, part, parts),
        out_shape=jax.ShapeDtypeStruct(density.shape, f32),
        in_specs=[spec] + [free] * len(tables),
        out_specs=free,
        scratch_shapes=[
            vmem((wide // LANES * rows_y * planes, LANES), f32),
            vmem((rows_y * planes, wide), f32),
            vmem((rows_y * planes, gy * slot), f32),
            vmem((rows_y * planes, wide), f32),
            vmem(density.shape, f32),
            vmem((parts, gy, rows_y, lanes), f32),
            vmem((parts, gy, rows_y, lanes), f32),
            vmem((rows, lanes), f32),
            vmem((parts, planes, rows, half), f32),
            vmem((planes, rows, half), f32),
            vmem((parts, rows, LANES), f32),
            vmem((parts, gz, part, LANES), f32),
            vmem((parts, gz, part, LANES), f32),
            vmem((parts, rows, LANES), f32),
            vmem((parts, gy, rows_y, lanes), f32),
            vmem((parts, gy, rows_y, lanes), f32),
            vmem((parts, rows, half), f32),
            vmem((parts, rows, half), f32),
            *[vmem(table.shape, jnp.bfloat16) for table in tables],
            dma((8,)), dma(()), dma((2,)),
            *[dma((parts, gy))] * 2,
            *[dma((parts, gz))] * 4,
            *[dma((parts, gy))] * 2,
        ],
        compiler_params=pltpu.CompilerParams(
            collective_id=0, has_side_effects=True, vmem_limit_bytes=60 * 1024 * 1024),
    )(density, *tables)


def solution(mesh):
    return jax.shard_map(
        on_device,
        mesh=mesh,
        in_specs=(P("gz", "gy"),),
        out_specs=P("gz", "gy"),
        check_vma=False,
    )
```

```python
import functools
import math

import jax
import jax.numpy as jnp
import numpy as np
from jax import lax
from jax.experimental import pallas as pl
from jax.experimental.pallas import tpu as pltpu
from jax.sharding import PartitionSpec as P

NX = 352
NY = 352
SCREEN = 128
LANES = 128
MESH = pl.DeviceIdType.MESH


def basis(length):
    j = np.arange(length)
    half = length // 2
    m = np.where(j <= half, j, j - half)
    angle = (m[:, None] * j[None, :] % length) * (2.0 * math.pi / length)
    rows = np.where(j[:, None] <= half, np.cos(angle), np.sin(angle))
    amp = np.where((j == 0) | (j == half), math.sqrt(1.0 / length), math.sqrt(2.0 / length))
    return rows * amp[:, None]


def split(value):
    high = value.astype(jnp.bfloat16)
    low = (value - high.astype(jnp.float32)).astype(jnp.bfloat16)
    return high, low


def dot3(a, b):
    dot = functools.partial(jnp.dot, preferred_element_type=jnp.float32)
    return dot(a[0], b[0]) + (dot(a[0], b[1]) + dot(a[1], b[0]))


def kappa_at(row, column):
    def wave(index, length):
        index = jnp.where(index <= length // 2, index, index - length // 2)
        return index.astype(jnp.float32) * (2.0 * math.pi / length)

    wave_y = wave(row, NY)
    wave_x = wave(column, NX)
    return jnp.sqrt(1.0 / (SCREEN * SCREEN) + wave_x * wave_x + wave_y * wave_y)


def kappa_of(rows, first_row, lanes, first_lane):
    row = lax.broadcasted_iota(jnp.int32, (rows, lanes), 0) + first_row
    column = lax.broadcasted_iota(jnp.int32, (rows, lanes), 1) + first_lane
    return kappa_at(row, column)


def kernel(planes, rows_y, gz, gy, part, parts, density, *refs):
    tables_hbm, refs = refs[:8], refs[8:]
    (out, rows_ref, slab, cols, acc, out_buf, send, recv, hat, seg, total, edge, edge_all, carry,
     carry_all, ends, send_back, back, decay_ref, scale_ref, *refs) = refs
    tables, refs = refs[:8], refs[8:]
    (table_sem, own_sem, out_sem, send_sem, recv_sem, edge_send, edge_recv, carry_send, carry_recv,
     back_send, back_recv) = refs
    fx, fx_low, ix, ix_low, fy, fy_low, iy, iy_low = tables
    width = NX // gy
    half = slot = LANES // 4
    fold = part // 2
    me_z = lax.axis_index("gz")
    me_y = lax.axis_index("gy")
    loads = []
    for i in range(8):
        load = pltpu.make_async_copy(tables_hbm[i], tables[i], table_sem.at[i])
        load.start()
        loads.append(load)
    barrier = pltpu.get_barrier_semaphore()
    for i in range(1, gy):
        pl.semaphore_signal(barrier, inc=1, device_id=(me_z, lax.rem(me_y + i, gy)), device_id_type=MESH)
    for i in range(1, gz):
        pl.semaphore_signal(barrier, inc=1, device_id=(lax.rem(me_z + i, gz), me_y), device_id_type=MESH)

    period = LANES // math.gcd(NX, LANES)
    stretch = period * NX
    steps = rows_y // period
    tall = rows_y * planes
    chunks = [min(LANES, NX - c) for c in range(0, NX, LANES)]

    def unpack(t, _):
        base = pl.multiple_of(t * stretch, LANES)
        values = density[:, pl.ds(base, stretch)]
        for q in range(period):
            row = pl.multiple_of((t * period + q) * planes, planes)
            for c, size in enumerate(chunks):
                start = q * NX + c * LANES
                rows_ref[pl.ds(c * tall + row, planes), :size] = values[:, start:start + size]
        return 0

    lax.fori_loop(0, steps, unpack, 0)
    for z in range(planes):
        for c, size in enumerate(chunks):
            slab[z * rows_y:(z + 1) * rows_y, c * LANES:c * LANES + size] = rows_ref[
                pl.ds(c * tall + z, rows_y, stride=planes), :][:, :size]
    group = 2

    def fill(h, which, value):
        for o in range(gz):
            for k in range(2):
                lane = (2 * k + which) * half
                row = o * part + k * fold
                edge[h, o, :, lane:lane + half] = value[row:row + fold]

    def take(h, which):
        for o in range(gz):
            for k in range(2):
                lane = (2 * k + which) * half
                row = o * part + k * fold
                ends[which, row:row + fold] = carry_all[h, o, :, lane:lane + half]
        return ends[which]

    def forward_x(h):
        for z0 in range(0, planes, group):
            block = slab[z0 * rows_y:(z0 + group) * rows_y, :NX]
            result = dot3(split(block), (fx[h], fx_low[h]))
            for z in range(z0, z0 + group):
                for p in range(gy):
                    send[h, p, :, z * half:(z + 1) * half] = result[
                        (z - z0) * rows_y:(z - z0 + 1) * rows_y, p * slot:p * slot + half]

    def exchange(source, target, h, sems, recvs):
        copies = []
        for i in list(range(2, gy)) + [1]:
            peer = lax.rem(me_y + i, gy)
            copy = pltpu.make_async_remote_copy(
                src_ref=source.at[h, peer], dst_ref=target.at[h, me_y],
                send_sem=sems.at[h, i], recv_sem=recvs.at[h, i],
                device_id=(me_z, peer), device_id_type=MESH)
            copy.start()
            copies.append(copy)
        own = pltpu.make_async_copy(source.at[h, me_y], target.at[h, me_y], own_sem)
        own.start()
        own.wait()
        return copies

    def arrive(copies):
        for copy in copies:
            copy.wait()

    def edges(h):
        lanes = planes * half
        hat[...] = dot3((fy[...], fy_low[...]), split(recv[h].reshape(gy * rows_y, lanes)))
        decay = decay_ref[h]
        value = None
        for z in range(planes):
            plane = hat[:, z * half:(z + 1) * half]
            seg[h, z] = plane
            value = plane if z == 0 else decay * value + plane
        fill(h, 0, value)
        for z in range(planes - 1, -1, -1):
            value = seg[h, z] if z == planes - 1 else decay * value + seg[h, z]
        fill(h, 1, value)
        copies = []
        for i in range(1, gz):
            peer = lax.rem(me_z + i, gz)
            copy = pltpu.make_async_remote_copy(
                src_ref=edge.at[h, peer],
                dst_ref=edge_all.at[h, me_z],
                send_sem=edge_send.at[h, i], recv_sem=edge_recv.at[h, i],
                device_id=(peer, me_y), device_id_type=MESH)
            copy.start()
            copies.append(copy)
        edge_all[h, me_z] = edge[h, me_z]
        return copies

    def carries(h):
        lane = lax.broadcasted_iota(jnp.int32, (fold, LANES), 1)
        row = lax.broadcasted_iota(jnp.int32, (fold, LANES), 0) + me_z * part
        row = jnp.where(lane >= 2 * half, row + fold, row)
        upward = (lane % (2 * half)) < half
        far = jnp.exp(-float(planes) * kappa_at(row, me_y * width + h * half + lane % half))
        value = jnp.zeros((fold, LANES), jnp.float32)
        for s in range(gz):
            carry[h, s] = value
            value = far * value + edge_all[h, s]
        value = jnp.zeros((fold, LANES), jnp.float32)
        for s in range(gz - 1, -1, -1):
            carry[h, s] = jnp.where(upward, carry[h, s], value)
            value = far * value + edge_all[h, s]
        copies = []
        for i in range(1, gz):
            peer = lax.rem(me_z + i, gz)
            copy = pltpu.make_async_remote_copy(
                src_ref=carry.at[h, peer], dst_ref=carry_all.at[h, me_z],
                send_sem=carry_send.at[h, i], recv_sem=carry_recv.at[h, i],
                device_id=(peer, me_y), device_id_type=MESH)
            copy.start()
            copies.append(copy)
        carry_all[h, me_z] = carry[h, me_z]
        return copies

    def inverse_y(h):
        decay = decay_ref[h]
        scale = scale_ref[h]
        value = take(h, 0)
        for z in range(planes):
            value = decay * value + seg[h, z]
            total[z] = value
        value = take(h, 1)
        for z in range(planes - 1, -1, -1):
            value = decay * value
            hat[:, z * half:(z + 1) * half] = (total[z] + value) * scale
            value = value + seg[h, z]
        result = dot3((iy[...], iy_low[...]), split(hat[...]))
        for p in range(gy):
            send_back[h, p] = result[p * rows_y:(p + 1) * rows_y]

    def inverse_x(h):
        for z0 in range(0, planes, group):
            for z in range(z0, z0 + group):
                for p in range(gy):
                    cols[z * rows_y:(z + 1) * rows_y, p * slot:p * slot + half] = back[
                        h, p, :, z * half:(z + 1) * half]
            block = pl.ds(z0 * rows_y, group * rows_y)
            result = dot3(split(cols[block, :]), (ix[h], ix_low[h]))
            if h > 0:
                result = result + acc[block, :]
            if h < parts - 1:
                acc[block, :] = result
                continue
            for z in range(z0, z0 + group):
                for c in range(len(chunks)):
                    rows_ref[pl.ds(c * tall + z, rows_y, stride=planes), :] = result[
                        (z - z0) * rows_y:(z - z0 + 1) * rows_y, c * LANES:(c + 1) * LANES]

    loads[0].wait()
    loads[1].wait()
    moving = []
    for h in range(parts):
        forward_x(h)
        if h == 0:
            pl.semaphore_wait(barrier, gy - 1 + gz - 1)
        moving.append(exchange(send, recv, h, send_sem, recv_sem))
    for h in range(parts):
        kappa = kappa_of(gz * part, 0, half, me_y * width + h * half)
        decay_ref[h] = jnp.exp(-kappa)
        scale_ref[h] = 0.5 / kappa
    for i in range(2, 8):
        loads[i].wait()
    sent = []
    for h in range(parts):
        arrive(moving[h])
        sent.append(edges(h))
    returned = []
    for h in range(parts):
        arrive(sent[h])
        returned.append(carries(h))
    moving = []
    for h in range(parts):
        arrive(returned[h])
        inverse_y(h)
        moving.append(exchange(send_back, back, h, back_send, back_recv))
    for h in range(parts):
        arrive(moving[h])
        inverse_x(h)

    def pack(t, _):
        pieces = []
        for q in range(period):
            row = pl.multiple_of((t * period + q) * planes, planes)
            for c, size in enumerate(chunks):
                pieces.append(rows_ref[pl.ds(c * tall + row, planes), :][:, :size])
        base = pl.multiple_of(t * stretch, LANES)
        out_buf[:, pl.ds(base, stretch)] = jnp.concatenate(pieces, axis=1)
        return 0

    stores = []
    cuts = [0, steps // 2, steps]
    for i in range(2):
        lax.fori_loop(cuts[i], cuts[i + 1], pack, 0)
        span = pl.ds(cuts[i] * stretch, (cuts[i + 1] - cuts[i]) * stretch)
        store = pltpu.make_async_copy(out_buf.at[:, span], out.at[:, span], out_sem.at[i])
        store.start()
        stores.append(store)
    for store in stores:
        store.wait()


def on_device(density):
    planes = density.shape[0]
    gz = lax.axis_size("gz")
    gy = lax.axis_size("gy")
    rows_y = NY // gy
    width = NX // gy
    half = slot = LANES // 4
    parts = -(-width // half)
    part = -(-NY // (16 * gz)) * 16
    rows = part * gz
    wide = -(-NX // LANES) * LANES
    forward_x = np.zeros((NX, gy, parts * half))
    forward_x[:, :, :width] = basis(NX).T.reshape(NX, gy, width)
    forward_x = forward_x.reshape(NX, gy, parts, half).transpose(2, 0, 1, 3)
    forward_x = forward_x.reshape(parts, NX, gy * slot)
    inverse_x = np.zeros((parts, gy * slot, wide))
    inverse_x[..., :NX] = forward_x.transpose(0, 2, 1)
    forward_y = np.zeros((rows, NY))
    forward_y[:NY] = basis(NY)
    tables = []
    for table in (forward_x, inverse_x, forward_y, forward_y.T):
        table = table.astype(np.float32)
        high = table.astype(jnp.bfloat16)
        low = (table - high.astype(np.float32)).astype(jnp.bfloat16)
        tables += [high, low]
    f32 = jnp.float32
    vmem = pltpu.VMEM
    dma = pltpu.SemaphoreType.DMA
    lanes = planes * half
    spec = pl.BlockSpec(memory_space=pltpu.VMEM)
    free = pl.BlockSpec(memory_space=pl.ANY)
    return pl.pallas_call(
        functools.partial(kernel, planes, rows_y, gz, gy, part, parts),
        out_shape=jax.ShapeDtypeStruct(density.shape, f32),
        in_specs=[spec] + [free] * len(tables),
        out_specs=free,
        scratch_shapes=[
            vmem((wide // LANES * rows_y * planes, LANES), f32),
            vmem((rows_y * planes, wide), f32),
            vmem((rows_y * planes, gy * slot), f32),
            vmem((rows_y * planes, wide), f32),
            vmem(density.shape, f32),
            vmem((parts, gy, rows_y, lanes), f32),
            vmem((parts, gy, rows_y, lanes), f32),
            vmem((rows, lanes), f32),
            vmem((parts, planes, rows, half), f32),
            vmem((planes, rows, half), f32),
            *[vmem((parts, gz, part // 2, LANES), f32)] * 4,
            vmem((2, rows, half), f32),
            vmem((parts, gy, rows_y, lanes), f32),
            vmem((parts, gy, rows_y, lanes), f32),
            vmem((parts, rows, half), f32),
            vmem((parts, rows, half), f32),
            *[vmem(table.shape, jnp.bfloat16) for table in tables],
            dma((8,)), dma(()), dma((2,)),
            *[dma((parts, gy))] * 2,
            *[dma((parts, gz))] * 4,
            *[dma((parts, gy))] * 2,
        ],
        compiler_params=pltpu.CompilerParams(
            collective_id=0, has_side_effects=True, vmem_limit_bytes=60 * 1024 * 1024),
    )(density, *tables)


def solution(mesh):
    return jax.shard_map(
        on_device,
        mesh=mesh,
        in_specs=(P("gz", "gy"),),
        out_specs=P("gz", "gy"),
        check_vma=False,
    )
```
